256 devices in a mesh: rep: 2 (over z), gx: 128 (over y, x, core).
Axes of the slice: x: 8, y: 8, z: 2, core: 2. Of those that a mesh axis runs over, the one named last changes fastest.
The devices are a block of a 8x8x16 slice.
Arguments:
- positions: float32 [3, 1048576], P(None, ('rep', 'gx')), parts along dimension 1, may hold values from 0 to 512, as said below
- polar: float32 [1048576], P(('rep', 'gx')), parts along dimension 0, may hold values from 0.25 to 1
- field_ext: float32 [3, 1048576], P(None, ('rep', 'gx')), parts along dimension 1, may hold values from -10 to 10
- tile_atom: int32 [1048576], P(('rep', 'gx')), parts along dimension 0, may hold values from 0 to 4095, as said below
- tile_list: int32 [8192, 3], P(('rep', 'gx')), parts along dimension 0, may hold values from 0 to 63, as said below
- image_shift: int32 [2, 8192, 3], P(None, ('rep', 'gx')), parts along dimension 1, may hold values from 0 to 1, as said below
Outputs:
- dipoles: float32 [3, 1048576], P(None, ('rep', 'gx')), parts along dimension 1
- residual: float32 [3, 1048576], P(None, ('rep', 'gx')), parts along dimension 1
The draws below stay inside these ranges and needn't reach their ends.
There are 2 independent parts, one for each index of `rep`. The reference program is written for one: setup_inputs(seed, part) draws one part's arguments, and reference() takes and returns one part's arrays. A program takes and returns all parts, laid end to end along the dimension named above; each array names one. Nothing has to cross between parts.
Inputs may be any that keep to these rules, and one draw needn't show every extreme that they name: `positions`: coordinates lie in a box of 512 by 128 by 64; the atoms of slab s have first coordinate between 4 s and 4 s + 4; no two atoms, and no atom and a periodic image of another, are closer than 1.4. `tile_atom`: for each slab, a permutation of 0 to 4095. `tile_list`: entry 0 of a tile is the tile's own index within its slab. Entry n of a tile of slab s names tile n of slab s if n < 32, else tile n - 32 of slab s + 1 (slab 0 after the last). `image_shift`: offsets along the second and third coordinates in box lengths, one pair for each entry of tile_list; zero for entry 0.
All inputs are finite; a program needn't handle non-finite values.
Results may differ from the reference program's by a relative error of at most 0.0003.
Values sent between devices are 32-bit elements; how exact they have to be, the bound alone decides.
No kernel may reach another device: no remote copies, remote signals or barrier semaphores. Data moves between devices by JAX's collectives and lax.ppermute only.
A program may use at most 64 MiB of HBM per device.

```python
import math
import jax
import jax.numpy as jnp
from jax import lax

TILE = 128
TILES_DEV = 32
NB = 3
ITERS = 4
TILES = 4096
ATOMS_DEV = 4096
ATOMS = 524288


def atom_order(key):
    slab_count = ATOMS // ATOMS_DEV
    keys = jax.random.split(jax.random.fold_in(key, 11), slab_count)

    def one_slab(slab_key):
        return jax.random.permutation(slab_key, ATOMS_DEV).astype(jnp.int32)
    return jax.vmap(one_slab)(keys).reshape(ATOMS)


def lattice_places():
    slot_ids = jnp.arange(ATOMS, dtype=jnp.int32)
    slab_ids = slot_ids // ATOMS_DEV
    local_ids = slot_ids % ATOMS_DEV
    tile_ids = local_ids // TILE
    within = local_ids % TILE
    rows_z = TILES_DEV // 8
    cell_y = tile_ids // rows_z
    cell_z = tile_ids % rows_z
    layer_id = within // 64
    along_y = within // 8 % 8
    along_z = within % 8
    coord_x = 4 * slab_ids + 2 * layer_id + 1
    coord_y = 2 * (8 * cell_y + along_y) + 1
    coord_z = 2 * (8 * cell_z + along_z) + 1
    return (jnp.stack([coord_x, coord_y, coord_z]).astype(jnp.float32), slab_ids)


def draw_tile_atom(key, part):
    return atom_order(key)


def draw_positions(key, part):
    order_ids = atom_order(key)
    base, slab_ids = lattice_places()
    jitter_key = jax.random.fold_in(key, 23)
    jitter = jax.random.uniform(jitter_key, (3, ATOMS), jnp.float32, -0.3, 0.3)
    placed = base + jitter
    target = slab_ids * ATOMS_DEV + order_ids
    return jnp.zeros((3, ATOMS), jnp.float32).at[:, target].set(placed)


def draw_field_ext(key, part):
    slab_count = ATOMS // ATOMS_DEV
    slab_ids = jnp.arange(ATOMS, dtype=jnp.int32) // ATOMS_DEV
    ramp = slab_ids.astype(jnp.float32) / (slab_count - 1)
    noise = jnp.clip(jax.random.normal(key, (3, ATOMS), jnp.float32), -5.0, 5.0)
    return noise * (0.6 + 1.2 * ramp)


def neighbour_entries(key):
    score_key = jax.random.fold_in(key, 37)
    scores = jax.random.randint(score_key, (TILES, 7), 0, 1 << 20) * 8 + jnp.arange(7, dtype=jnp.int32)[None, :]
    picked = jnp.argsort(scores, axis=1)[:, :NB - 1].astype(jnp.int32) + 1
    step_x = picked // 4
    step_y = picked // 2 % 2
    step_z = picked % 2
    rows_z = TILES_DEV // 8
    tile_ids = jnp.arange(TILES, dtype=jnp.int32) % TILES_DEV
    cell_y = (tile_ids // rows_z)[:, None]
    cell_z = (tile_ids % rows_z)[:, None]
    next_y = cell_y + step_y
    next_z = cell_z + step_z
    image_y = next_y // 8
    image_z = next_z // rows_z
    named = step_x * TILES_DEV + next_y % 8 * rows_z + next_z % rows_z
    lists = jnp.concatenate([tile_ids[:, None], named], axis=1).astype(jnp.int32)
    zeros_col = jnp.zeros((TILES, 1), jnp.int32)
    shifts = jnp.stack([jnp.concatenate([zeros_col, image_y], axis=1), jnp.concatenate([zeros_col, image_z], axis=1)]).astype(jnp.int32)
    return (lists, shifts)


def draw_tile_list(key, part):
    lists, shifts = neighbour_entries(key)
    return lists


def draw_image_shift(key, part):
    lists, shifts = neighbour_entries(key)
    return shifts


def shard_levels(own_key, shape, cuts, least, largest):
    factor_of = 1.0
    for position, blocks in cuts:
        steps = jax.random.uniform(jax.random.fold_in(jax.random.fold_in(own_key, 6), position), (blocks,), jnp.float32, least / len(cuts), largest / len(cuts))
        factor_of = factor_of * jnp.repeat(jnp.exp(steps), shape[position] // blocks).reshape((-1,) + (1,) * (len(shape) - 1 - position))
    return factor_of


def setup_inputs(seed: int = 0, part: int = 0) -> dict:
    splits = jax.random.split(jax.random.key(seed), 7)
    part_splits = jax.random.split(jax.random.fold_in(splits[6], part), 7)
    positions = draw_positions(jax.random.fold_in(jax.random.fold_in(splits[6], part), 71), part)
    polar = jnp.clip(jnp.exp(math.log(1.0) - 1.3862944 * jax.random.uniform(part_splits[1], (ATOMS,), jnp.float32) ** shard_levels(part_splits[1], (ATOMS,), ((0, 128),), -0.2, 0.2)), 0.25, 1.0)
    field_ext = draw_field_ext(jax.random.fold_in(jax.random.fold_in(splits[6], part), 71), part)
    tile_atom = draw_tile_atom(jax.random.fold_in(jax.random.fold_in(splits[6], part), 71), part)
    tile_list = draw_tile_list(jax.random.fold_in(jax.random.fold_in(splits[6], part), 71), part)
    image_shift = draw_image_shift(jax.random.fold_in(jax.random.fold_in(splits[6], part), 71), part)
    return {"positions": positions, "polar": polar, "field_ext": field_ext, "tile_atom": tile_atom, "tile_list": tile_list, "image_shift": image_shift}


thole_factor = 0.39

def pair_block(place_left, root_left, moment_left, place_right, root_right, moment_right, weights, self_flags):
    offset_x = place_right[:, 0, None, :] - place_left[:, 0, :, None]
    offset_y = place_right[:, 1, None, :] - place_left[:, 1, :, None]
    offset_z = place_right[:, 2, None, :] - place_left[:, 2, :, None]
    dist_sq = offset_x * offset_x + offset_y * offset_y + offset_z * offset_z
    tile_width = place_left.shape[2]
    row_ids = lax.broadcasted_iota(jnp.int32, (tile_width, tile_width), 0)
    column_ids = lax.broadcasted_iota(jnp.int32, (tile_width, tile_width), 1)
    same_atom = jnp.logical_and(self_flags[:, None, None] > 0, (row_ids == column_ids)[None])
    dist_sq = jnp.where(same_atom, 1.0, dist_sq)
    inv_dist = lax.rsqrt(dist_sq)
    distance = dist_sq * inv_dist
    damp_arg = thole_factor * dist_sq * distance / (root_left[:, :, None] * root_right[:, None, :])
    decay = jnp.exp(-damp_arg)
    inv_cube = jnp.where(same_atom, 0.0, weights[:, None, None] * inv_dist * inv_dist * inv_dist)
    coeff_three = (1.0 - decay) * inv_cube
    coeff_five = 3.0 * (1.0 - (1.0 + damp_arg) * decay) * inv_cube * inv_dist * inv_dist
    offsets = (offset_x, offset_y, offset_z)
    proj_right = offset_x * moment_right[:, 0, None, :] + offset_y * moment_right[:, 1, None, :] + offset_z * moment_right[:, 2, None, :]
    proj_left = offset_x * moment_left[:, 0, :, None] + offset_y * moment_left[:, 1, :, None] + offset_z * moment_left[:, 2, :, None]
    lift_right = coeff_five * proj_right
    lift_left = coeff_five * proj_left
    field_left = jnp.stack([lax.optimization_barrier(jnp.sum(lift_right * offsets[component] - coeff_three * moment_right[:, component, None, :], axis=2)) for component in range(3)], axis=1)
    field_right = jnp.stack([lax.optimization_barrier(jnp.sum(lift_left * offsets[component] - coeff_three * moment_left[:, component, :, None], axis=1)) for component in range(3)], axis=1)
    return (field_left, field_right)

def slab_fields(window_place, window_root, window_moment, left_index, right_index, image_vec, weights, self_flags):
    entries = left_index.shape[0]
    block_size = math.gcd(entries, 32)
    window_size = window_place.shape[0]
    tile_width = window_place.shape[2]
    slot_ids = jnp.arange(window_size, dtype=jnp.int32)

    def accumulate(summed, first_entry):
        left_rows = lax.dynamic_slice_in_dim(left_index, first_entry, block_size)
        right_rows = lax.dynamic_slice_in_dim(right_index, first_entry, block_size)
        image_rows = lax.dynamic_slice_in_dim(image_vec, first_entry, block_size)
        weight_rows = lax.dynamic_slice_in_dim(weights, first_entry, block_size)
        flag_rows = lax.dynamic_slice_in_dim(self_flags, first_entry, block_size)
        place_left = jnp.take(window_place, left_rows, axis=0)
        place_right = jnp.take(window_place, right_rows, axis=0) + image_rows[:, :, None]
        field_left, field_right = pair_block(place_left, jnp.take(window_root, left_rows, axis=0), jnp.take(window_moment, left_rows, axis=0), place_right, jnp.take(window_root, right_rows, axis=0), jnp.take(window_moment, right_rows, axis=0), weight_rows, flag_rows)
        hit_left = (left_rows[:, None] == slot_ids[None, :]).astype(jnp.float32)
        hit_right = (right_rows[:, None] == slot_ids[None, :]).astype(jnp.float32)
        summed = summed + jnp.einsum('ew,ef->wf', hit_left, field_left.reshape(block_size, 3 * tile_width), precision=lax.Precision.HIGHEST)
        summed = summed + jnp.einsum('ew,ef->wf', hit_right, field_right.reshape(block_size, 3 * tile_width), precision=lax.Precision.HIGHEST)
        return (summed, None)
    first_entries = jnp.arange(0, entries, block_size, dtype=jnp.int32)
    summed, _ = lax.scan(accumulate, jnp.zeros((window_size, 3 * tile_width), jnp.float32), first_entries)
    return summed.reshape(window_size, 3, tile_width)

def image_vectors(lists, shifts, last_flag, tile_count, box_x, box_y, box_z):
    crossing = lists >= tile_count
    wrapped = jnp.where(jnp.logical_and(crossing, last_flag), box_x, 0.0)
    vectors = jnp.stack([wrapped, shifts[0].astype(jnp.float32) * box_y, shifts[1].astype(jnp.float32) * box_z], axis=-1)
    return vectors.reshape(-1, 3)

def reference(positions, polar, field_ext, tile_atom, tile_list, image_shift):
    slab_count = TILES // TILES_DEV
    slot_atom = jnp.arange(ATOMS, dtype=jnp.int32) // ATOMS_DEV * ATOMS_DEV + tile_atom
    tiled_place = positions[:, slot_atom].reshape(3, TILES, TILE).transpose(1, 0, 2)
    tiled_polar = polar[slot_atom].reshape(TILES, TILE)
    tiled_root = jnp.sqrt(tiled_polar)
    tiled_rhs = field_ext[:, slot_atom].reshape(3, TILES, TILE).transpose(1, 0, 2)
    box_x = 4.0 * slab_count
    box_y = 128.0
    box_z = 2.0 * TILES_DEV
    last_flag = (jnp.arange(TILES, dtype=jnp.int32) // TILES_DEV == slab_count - 1)[:, None]
    image_all = image_vectors(tile_list, image_shift, last_flag, TILES_DEV, box_x, box_y, box_z)
    entry_ids = jnp.arange(NB, dtype=jnp.int32)
    own_left = jnp.repeat(jnp.arange(TILES_DEV, dtype=jnp.int32), NB)
    own_weights = jnp.tile(jnp.where(entry_ids == 0, 0.5, 1.0), TILES_DEV)
    own_self = jnp.tile((entry_ids == 0).astype(jnp.int32), TILES_DEV)
    slab_ids = jnp.arange(slab_count, dtype=jnp.int32)

    def apply_operator(moment):

        def per_slab(summed, slab):
            first = slab * TILES_DEV
            after = (slab + 1) % slab_count * TILES_DEV
            window_place = jnp.concatenate([lax.dynamic_slice_in_dim(tiled_place, first, TILES_DEV), lax.dynamic_slice_in_dim(tiled_place, after, TILES_DEV)], axis=0)
            window_root = jnp.concatenate([lax.dynamic_slice_in_dim(tiled_root, first, TILES_DEV), lax.dynamic_slice_in_dim(tiled_root, after, TILES_DEV)], axis=0)
            window_moment = jnp.concatenate([lax.dynamic_slice_in_dim(moment, first, TILES_DEV), lax.dynamic_slice_in_dim(moment, after, TILES_DEV)], axis=0)
            lists = lax.dynamic_slice_in_dim(tile_list, first, TILES_DEV).reshape(-1)
            images = lax.dynamic_slice_in_dim(image_all, first * NB, TILES_DEV * NB)
            window = slab_fields(window_place, window_root, window_moment, own_left, lists, images, own_weights, own_self)
            summed = lax.dynamic_update_slice_in_dim(summed, lax.dynamic_slice_in_dim(summed, first, TILES_DEV) + window[:TILES_DEV], first, 0)
            summed = lax.dynamic_update_slice_in_dim(summed, lax.dynamic_slice_in_dim(summed, after, TILES_DEV) + window[TILES_DEV:], after, 0)
            return (summed, None)
        fields, _ = lax.scan(per_slab, jnp.zeros((TILES, 3, TILE), jnp.float32), slab_ids)
        return moment / tiled_polar[:, None, :] - fields
    solution = jnp.zeros_like(tiled_rhs)
    resid = tiled_rhs
    direction = tiled_rhs
    norm_now = jnp.sum(resid * resid)
    for iteration in range(ITERS):
        applied = apply_operator(direction)
        step_size = norm_now / jnp.sum(direction * applied)
        solution = solution + step_size * direction
        resid = resid - step_size * applied
        norm_next = jnp.sum(resid * resid)
        direction = resid + norm_next / norm_now * direction
        norm_now = norm_next
    dipoles = jnp.zeros((3, ATOMS), jnp.float32).at[:, slot_atom].set(solution.transpose(1, 0, 2).reshape(3, ATOMS))
    residual = jnp.zeros((3, ATOMS), jnp.float32).at[:, slot_atom].set(resid.transpose(1, 0, 2).reshape(3, ATOMS))
    return (dipoles, residual)
```

```python
import functools

import jax
import jax.numpy as jnp
from jax import lax
from jax.experimental import pallas as pl
from jax.experimental.pallas import tpu as pltpu
from jax.sharding import PartitionSpec as P

ITERS = 4
REP_GX = ("rep", "gx")
THOLE = 0.39
SHIFT = 2.5
SCALE = 1.5
MATS = 4
SLOTS = 10
MIB = 2**20

F32 = jnp.float32
VMEM = pl.BlockSpec(memory_space=pltpu.VMEM)
SMEM = pl.BlockSpec(memory_space=pltpu.SMEM)
HBM = pl.BlockSpec(memory_space=pltpu.MemorySpace.HBM)


def spread(row, height=8):
    return jnp.broadcast_to(row, (height, row.shape[1]))


def lane_pick(row_block, lanes):
    return jnp.take_along_axis(row_block, lanes, axis=1)


def params(mib):
    return pltpu.CompilerParams(vmem_limit_bytes=mib * MIB)


def tile_in_kernel(pos_ref, pol_ref, fld_ref, idx_ref, out_ref):
    tiles = idx_ref.shape[0]
    width = idx_ref.shape[1]
    for q in range(tiles // 8):
        rows = idx_ref[8 * q : 8 * q + 8, :]
        high = rows // width
        low = rows - high * width

        def step(h, acc):
            at = pl.ds(pl.multiple_of(h * width, width), width)
            hit = high == h
            new = []
            for c in range(7):
                if c < 3:
                    row = pos_ref[c : c + 1, at]
                elif c == 3:
                    row = pol_ref[0:1, at]
                else:
                    row = fld_ref[c - 4 : c - 3, at]
                new.append(jnp.where(hit, lane_pick(spread(row), low), acc[c]))
            return tuple(new)

        acc = lax.fori_loop(0, tiles, step, (jnp.zeros((8, width), F32),) * 7, unroll=4)
        values = list(acc[:3]) + [lax.rsqrt(acc[3])] + list(acc[4:]) + [1.0 / acc[3]]
        for c in range(8):
            out_ref[c * tiles + 8 * q : c * tiles + 8 * q + 8, :] = values[c]


def inverse_kernel(idx_ref, out_ref):
    tiles, width = idx_ref.shape
    total = jnp.zeros((2 * tiles, width), F32)
    lane = lax.broadcasted_iota(jnp.int32, (tiles, width), 1).astype(F32)
    row_id = lax.broadcasted_iota(jnp.int32, (tiles, width), 0)
    low_id = lax.broadcasted_iota(jnp.int32, (width, width), 0)
    for t in range(tiles):
        row = idx_ref[t : t + 1, :]
        high = row // width
        low = row - high * width
        hit = spread(high, tiles) == row_id
        left = jnp.concatenate([jnp.where(hit, float(t), 0.0), jnp.where(hit, lane, 0.0)], axis=0)
        right = jnp.where(spread(low, width) == low_id, 1.0, 0.0)
        total = total + lax.dot_general(
            left.astype(jnp.bfloat16),
            right.astype(jnp.bfloat16),
            (((1,), (1,)), ((), ())),
            preferred_element_type=F32,
        )
    out_ref[...] = (total[:tiles] * float(width) + total[tiles:] + 0.5).astype(jnp.int32)


def take_neighbours(par, near_ref, far_ref, nb_ref, start, rows):
    nb_ref[pl.ds(pl.multiple_of(par * rows, 8), rows), :] = near_ref[start : start + rows, :]
    nb_ref[pl.ds(pl.multiple_of((1 - par) * rows, 8), rows), :] = far_ref[start : start + rows, :]


def pair_coefficients(off, ci, rj, same):
    dist_sq = off[0] * off[0] + off[1] * off[1] + off[2] * off[2]
    if same is not None:
        dist_sq = jnp.where(same, 1.0, dist_sq)
    inv = lax.rsqrt(dist_sq)
    damp = (dist_sq * (dist_sq * inv)) * (ci * rj)
    decay = jnp.exp(-damp)
    inv_sq = inv * inv
    cube = inv_sq * inv
    g3 = (1.0 - decay) * cube
    g5 = (3.0 - (3.0 + 3.0 * damp) * decay) * (cube * inv_sq)
    root = g5 * lax.rsqrt(g5)
    if same is not None:
        g3 = jnp.where(same, 0.0, g3)
        root = jnp.where(same, 0.0, root)
    return [root * off[0], root * off[1], root * off[2], g3]


def pairs_kernel(
    par_ref, own_list, prev_list, own_ref, near_ref, far_ref,
    tensor_ref, prev_hbm, tab_ref, nb_ref, col_ref, out_slots, sems,
    *, boxes,
):
    tiles = own_ref.shape[0] // 8
    width = own_ref.shape[1]
    par = par_ref[0]
    wrap_next = par_ref[1].astype(F32) * boxes[0]
    wrap_prev = par_ref[2].astype(F32) * boxes[0]
    rows = 4 * tiles
    take_neighbours(par, near_ref, far_ref, nb_ref, 0, rows)
    links = own_list.shape[1] // tiles
    extra = links - 1
    cap = extra * tiles

    def sort_own(k, counts):
        inner, outer = counts
        t = k // extra
        at = t * links + 1 + (k - t * extra)
        n = own_list[0, at]
        tab_ref[1, inner] = k
        tab_ref[2, outer] = k
        near = (n < tiles).astype(jnp.int32)
        return inner + near, outer + 1 - near

    inner, outer = lax.fori_loop(0, cap, sort_own, (jnp.int32(0), jnp.int32(0)))

    def sort_prev(k, count):
        t = k // extra
        at = t * links + 1 + (k - t * extra)
        n = prev_list[0, at]
        tab_ref[3, count] = k
        return count + (n >= tiles).astype(jnp.int32)

    behind = lax.fori_loop(0, cap, sort_prev, jnp.int32(0))
    tab_ref[0, 0] = inner
    tab_ref[0, 1] = outer
    tab_ref[0, 2] = behind

    def columns(t, _):
        for c in range(4):
            row = own_ref[pl.ds(c * tiles + t, 1), :]
            if c == 3:
                row = row * THOLE
            col_ref[pl.ds(pl.multiple_of((t * 4 + c) * width, width), width), :] = spread(row, width).T
        return 0

    lax.fori_loop(0, tiles, columns, 0)
    chunks = width // 8

    def block(own_tile, row, store, same, lead):
        for k in range(chunks):
            base = pl.multiple_of(own_tile * 4 * width, width)
            col = [col_ref[pl.ds(base + c * width + 8 * k, 8), :] for c in range(4)]
            if lead is not None:
                off = [(col[c] + lead[c]) - row[c] for c in range(3)]
            else:
                off = [row[c] - col[c] for c in range(3)]
            mask = None
            if same:
                i = lax.broadcasted_iota(jnp.int32, (8, width), 0) + 8 * k
                j = lax.broadcasted_iota(jnp.int32, (8, width), 1)
                mask = i == j
            store(k, pair_coefficients(off, col[3], row[3], mask))

    def store_own(slot):
        def store(k, mats):
            for m in range(MATS):
                at = pl.multiple_of((slot * MATS + m) * width, width) + 8 * k
                tensor_ref[pl.ds(at, 8), :] = mats[m]

        return store

    def own_rows(n):
        return [spread(own_ref[pl.ds(c * tiles + n, 1), :]) for c in range(4)]

    def nb_rows(side, n):
        return [spread(nb_ref[pl.ds(side * rows + c * tiles + n, 1), :]) for c in range(4)]

    def self_job(t, _):
        block(t, own_rows(t), store_own(t), True, None)
        return 0

    lax.fori_loop(0, tiles, self_job, 0)

    def shifts(lists, at):
        return lists[1, at].astype(F32) * boxes[1], lists[2, at].astype(F32) * boxes[2]

    def shifted(row, lead):
        return [row[c] + lead[c] for c in range(3)] + [row[3]]

    def inner_job(i, _):
        k = tab_ref[1, i]
        t = k // extra
        at = t * links + 1 + (k - t * extra)
        n = own_list[0, at]
        y, z = shifts(own_list, at)
        block(t, shifted(own_rows(n), (0.0, y, z)), store_own(tiles + k), False, None)
        return 0

    lax.fori_loop(0, inner, inner_job, 0)

    def outer_job(i, _):
        k = tab_ref[2, i]
        t = k // extra
        at = t * links + 1 + (k - t * extra)
        n = own_list[0, at] - tiles
        y, z = shifts(own_list, at)
        block(t, shifted(nb_rows(0, n), (wrap_next, y, z)), store_own(tiles + k), False, None)
        return 0

    lax.fori_loop(0, outer, outer_job, 0)

    def out_copy(i):
        slot = lax.rem(i, 2)
        size = MATS * width
        return pltpu.make_async_copy(
            out_slots.at[pl.ds(pl.multiple_of(slot * size, size), size), :],
            prev_hbm.at[pl.ds(pl.multiple_of(i * size, size), size), :],
            sems.at[slot],
        )

    def behind_job(i, _):
        k = tab_ref[3, i]
        t = k // extra
        at = t * links + 1 + (k - t * extra)
        n = prev_list[0, at] - tiles
        y, z = shifts(prev_list, at)

        @pl.when(i >= 2)
        def _():
            out_copy(i - 2).wait()

        base = pl.multiple_of(lax.rem(i, 2) * MATS * width, width)

        def store(c, mats):
            for m in range(MATS):
                out_slots[pl.ds(base + m * width + 8 * c, 8), :] = mats[m]

        block(n, nb_rows(1, t), store, False, (wrap_prev, y, z))
        out_copy(i).start()
        return 0

    lax.fori_loop(0, behind, behind_job, 0)

    @pl.when(behind >= 2)
    def _():
        out_copy(behind - 2).wait()

    @pl.when(behind >= 1)
    def _():
        out_copy(behind - 1).wait()


def apply_kernel(
    par_ref, tab_ref, own_list, prev_list, tensor_ref, prev_hbm, own_ref, near_ref, far_ref, inv_ref,
    out_ref, nb_ref, left_ref, right_ref, slots_ref, sems,
    *, start, inv_start,
):
    width = own_ref.shape[1]
    rows = out_ref.shape[0]
    tiles = rows // 3
    links = own_list.shape[1] // tiles
    extra = links - 1
    par = par_ref[0]
    inner = tab_ref[0, 0]
    outer = tab_ref[0, 1]
    behind = tab_ref[0, 2]
    chunks = width // 8
    size = MATS * width

    def in_copy(i):
        slot = lax.rem(i, SLOTS)
        return pltpu.make_async_copy(
            prev_hbm.at[pl.ds(pl.multiple_of(i * size, size), size), :],
            slots_ref.at[pl.ds(pl.multiple_of(slot * size, size), size), :],
            sems.at[slot],
        )

    def begin(i, _):
        in_copy(i).start()
        return 0

    lax.fori_loop(0, jnp.minimum(behind, SLOTS), begin, 0)
    take_neighbours(par, near_ref, far_ref, nb_ref, start, rows)
    right_ref[...] = jnp.zeros_like(right_ref)

    def own_rows(n):
        return [spread(own_ref[pl.ds(start + c * tiles + n, 1), :]) for c in range(3)]

    def nb_rows(side, n):
        return [spread(nb_ref[pl.ds(side * rows + c * tiles + n, 1), :]) for c in range(3)]

    def left_at(tile, c, k):
        return pl.ds(pl.multiple_of((tile * 3 + c) * width, width) + 8 * k, 8)

    def one_side(source, base, tile, row, fresh):
        for k in range(chunks):
            s = [source[pl.ds(base + m * width + 8 * k, 8), :] for m in range(MATS)]
            lift = s[0] * row[0] + s[1] * row[1] + s[2] * row[2]
            for c in range(3):
                value = s[c] * lift - s[3] * row[c]
                if not fresh:
                    value = left_ref[left_at(tile, c, k), :] + value
                left_ref[left_at(tile, c, k), :] = value

    def self_job(t, _):
        one_side(tensor_ref, pl.multiple_of(t * size, size), t, own_rows(t), True)
        return 0

    lax.fori_loop(0, tiles, self_job, 0)

    def inner_job(i, _):
        k = tab_ref[1, i]
        t = k // extra
        n = own_list[0, t * links + 1 + (k - t * extra)]
        base = pl.multiple_of((tiles + k) * size, size)
        row = own_rows(n)
        col = [spread(own_ref[pl.ds(start + c * tiles + t, 1), :], width).T for c in range(3)]
        acc = [right_ref[pl.ds(pl.multiple_of((n * 3 + c) * 8, 8), 8), :] for c in range(3)]
        for q in range(chunks):
            s = [tensor_ref[pl.ds(base + m * width + 8 * q, 8), :] for m in range(MATS)]
            lift = s[0] * row[0] + s[1] * row[1] + s[2] * row[2]
            for c in range(3):
                at = left_at(t, c, q)
                left_ref[at, :] = left_ref[at, :] + (s[c] * lift - s[3] * row[c])
            mine = [col[c][8 * q : 8 * q + 8, :] for c in range(3)]
            lift = s[0] * mine[0] + s[1] * mine[1] + s[2] * mine[2]
            for c in range(3):
                acc[c] = acc[c] + (s[c] * lift - s[3] * mine[c])
        for c in range(3):
            right_ref[pl.ds(pl.multiple_of((n * 3 + c) * 8, 8), 8), :] = acc[c]
        return 0

    lax.fori_loop(0, inner, inner_job, 0)

    def outer_job(i, _):
        k = tab_ref[2, i]
        t = k // extra
        n = own_list[0, t * links + 1 + (k - t * extra)] - tiles
        one_side(tensor_ref, pl.multiple_of((tiles + k) * size, size), t, nb_rows(0, n), False)
        return 0

    lax.fori_loop(0, outer, outer_job, 0)

    def behind_job(i, _):
        k = tab_ref[3, i]
        t = k // extra
        n = prev_list[0, t * links + 1 + (k - t * extra)] - tiles
        in_copy(i).wait()
        slot = lax.rem(i, SLOTS)
        one_side(slots_ref, pl.multiple_of(slot * size, size), n, nb_rows(1, t), False)

        @pl.when(i + SLOTS < behind)
        def _():
            in_copy(i + SLOTS).start()

        return 0

    lax.fori_loop(0, behind, behind_job, 0)

    def finish(t, _):
        weight = (inv_ref[pl.ds(inv_start + t, 1), :] - SHIFT) * (1.0 / SCALE)
        for c in range(3):
            block = left_ref[pl.ds(pl.multiple_of((t * 3 + c) * width, width), width), :].T
            field = jnp.sum(block, axis=0, keepdims=True) + jnp.sum(
                right_ref[pl.ds(pl.multiple_of((t * 3 + c) * 8, 8), 8), :], axis=0, keepdims=True
            )
            mine = own_ref[pl.ds(start + c * tiles + t, 1), :]
            out_ref[pl.ds(c * tiles + t, 1), :] = mine * weight - field * (1.0 / SCALE)
        return 0

    lax.fori_loop(0, tiles, finish, 0, unroll=2)


PAIRS = [(i, j) for i in range(ITERS + 1) for j in range(i, ITERS + 1)]


def gram_kernel(*refs, start):
    vectors, out_ref = refs[:-1], refs[-1]
    rows, width = vectors[-1].shape
    lane = lax.broadcasted_iota(jnp.int32, (1, width), 1)
    total = jnp.zeros((1, width), F32)
    starts = (start,) + (0,) * ITERS
    for n, (i, j) in enumerate(PAIRS):
        product = vectors[i][starts[i] : starts[i] + rows, :] * vectors[j][starts[j] : starts[j] + rows, :]
        line = jnp.sum(product, axis=0, keepdims=True)
        total = jnp.where(lane == n, jnp.sum(line, axis=1, keepdims=True), total)
    out_ref[...] = total


def output_kernel(parts_ref, inv_ref, *refs, start):
    vectors, (dip_ref, res_ref, mix_ref) = refs[: ITERS + 1], refs[ITERS + 1 :]
    rows, width = vectors[-1].shape
    tiles = rows // 3
    sums = jnp.sum(parts_ref[...], axis=0, keepdims=True)
    lane = lax.broadcasted_iota(jnp.int32, (1, width), 1)
    gram = {}
    for n, (i, j) in enumerate(PAIRS):
        value = jnp.sum(jnp.where(lane == n, sums, 0.0), axis=1, keepdims=True)
        gram[i, j] = gram[j, i] = jnp.broadcast_to(value, (8, width))
    zero = jnp.zeros((8, width), F32)

    def add(a, b):
        return b if a is None else a if b is None else a + b

    def inner(a, b):
        total = None
        for i in range(ITERS + 1):
            for j in range(ITERS + 1):
                if a[i] is not None and b[j] is not None:
                    total = add(total, a[i] * b[j] * gram[i, j])
        return total

    def operate(a):
        out = [None if v is None else SHIFT * v for v in a]
        for i in range(ITERS):
            if a[i] is not None:
                out[i + 1] = add(out[i + 1], SCALE * a[i])
        return out

    x = [None] * (ITERS + 1)
    r = [zero + 1.0] + [None] * ITERS
    d = list(r)
    norm = inner(r, r)
    for step in range(ITERS):
        q = operate(d)
        size = norm / inner(d, q)
        x = [add(x[k], None if d[k] is None else size * d[k]) for k in range(ITERS + 1)]
        r = [add(r[k], None if q[k] is None else -size * q[k]) for k in range(ITERS + 1)]
        if step + 1 < ITERS:
            new = inner(r, r)
            ratio = new / norm
            d = [add(r[k], None if d[k] is None else ratio * d[k]) for k in range(ITERS + 1)]
            norm = new
    starts = (start,) + (0,) * ITERS
    for b in range(rows // 8):
        for which, weights in enumerate((x, r)):
            total = None
            for k in range(ITERS + 1):
                if weights[k] is not None:
                    total = add(total, weights[k] * vectors[k][starts[k] + 8 * b : starts[k] + 8 * b + 8, :])
            mix_ref[which * rows + 8 * b : which * rows + 8 * b + 8, :] = total
    for q in range(tiles // 8):
        index = inv_ref[8 * q : 8 * q + 8, :]
        high = index // width
        low = index - high * width

        def step(h, acc):
            hit = high == h
            return tuple(
                jnp.where(hit, lane_pick(spread(mix_ref[pl.ds(c * tiles + h, 1), :]), low), acc[c])
                for c in range(6)
            )

        acc = lax.fori_loop(0, tiles, step, (zero,) * 6, unroll=4)
        for c in range(6):
            out = dip_ref if c < 3 else res_ref
            for s in range(8):
                at = (8 * q + s) * width
                out[c % 3 : c % 3 + 1, at : at + width] = acc[c][s : s + 1, :]


def shape(rows, width, dtype=F32):
    return jax.ShapeDtypeStruct((rows, width), dtype)


def on_device(positions, polar, field_ext, tile_atom, tile_list, image_shift):
    tiles, links = tile_list.shape
    atoms = tile_atom.shape[0]
    width = atoms // tiles
    slabs = lax.axis_size("gx")
    slab = lax.axis_index("gx")
    rows = 3 * tiles
    cap = tiles * (links - 1)
    boxes = (4.0 * slabs, 128.0, 2.0 * tiles)
    near_pairs = [(i, i ^ 1) for i in range(slabs)]
    far_pairs = [(i, ((i + 1) ^ 1) - 1 if 0 < i < slabs - 1 else slabs - 1 - i) for i in range(slabs)]

    def swap(value):
        return lax.ppermute(value, "gx", near_pairs), lax.ppermute(value, "gx", far_pairs)

    lists = jnp.concatenate(
        [tile_list.reshape(1, -1), image_shift.reshape(2, -1)], axis=0
    )
    prev_lists = lax.ppermute(lists, "gx", [(i, (i + 1) % slabs) for i in range(slabs)])
    par = jnp.stack(
        [slab % 2, (slab == slabs - 1).astype(jnp.int32), (slab == 0).astype(jnp.int32)]
    ).astype(jnp.int32)
    index = tile_atom.reshape(tiles, width)
    packed = pl.pallas_call(
        tile_in_kernel,
        out_shape=shape(8 * tiles, width),
        in_specs=[VMEM] * 4,
        out_specs=VMEM,
        compiler_params=params(4),
        name="tile_in",
    )(positions, polar.reshape(1, -1), field_ext, index)
    inverse = pl.pallas_call(
        inverse_kernel,
        out_shape=shape(tiles, width, jnp.int32),
        in_specs=[VMEM],
        out_specs=VMEM,
        compiler_params=params(4),
        cost_estimate=pl.CostEstimate(flops=4_000_000, bytes_accessed=32768, transcendentals=0),
        name="inverse",
    )(index)
    near, far = swap(packed)
    tensor, prev_tensor, table = pl.pallas_call(
        functools.partial(pairs_kernel, boxes=boxes),
        out_shape=(
            pltpu.VMEM(((tiles + cap) * MATS * width, width), F32),
            pltpu.MemorySpace.HBM((cap * MATS * width, width), F32),
            shape(4, cap + 1, jnp.int32),
        ),
        in_specs=[SMEM] * 3 + [VMEM] * 3,
        out_specs=(VMEM, HBM, SMEM),
        scratch_shapes=[
            pltpu.VMEM((2 * 4 * tiles, width), F32),
            pltpu.VMEM((4 * tiles * width, width), F32),
            pltpu.VMEM((2 * MATS * width, width), F32),
            pltpu.SemaphoreType.DMA((2,)),
        ],
        compiler_params=params(10),
        name="pairs",
    )(par, lists, prev_lists, packed, near, far)

    prev_tensor = pltpu.with_memory_space_constraint(prev_tensor, pltpu.MemorySpace.HBM)

    def apply(vector, near, far, start):
        return pl.pallas_call(
            functools.partial(apply_kernel, start=start, inv_start=7 * tiles),
            out_shape=shape(rows, width),
            in_specs=[SMEM] * 4 + [VMEM, HBM] + [VMEM] * 4,
            out_specs=VMEM,
            scratch_shapes=[
                pltpu.VMEM((2 * rows, width), F32),
                pltpu.VMEM((rows * width, width), F32),
                pltpu.VMEM((8 * rows, width), F32),
                pltpu.VMEM((SLOTS * MATS * width, width), F32),
                pltpu.SemaphoreType.DMA((SLOTS,)),
            ],
            compiler_params=params(10),
            name="apply",
        )(par, table, lists, prev_lists, tensor, prev_tensor, vector, near, far, packed)

    start = 4 * tiles
    basis = [packed]
    vector = apply(packed, near, far, start)
    basis.append(vector)
    for _ in range(ITERS - 1):
        near, far = swap(vector)
        vector = apply(vector, near, far, 0)
        basis.append(vector)
    gram = pl.pallas_call(
        functools.partial(gram_kernel, start=start),
        out_shape=shape(1, width),
        in_specs=[VMEM] * (ITERS + 1),
        out_specs=VMEM,
        compiler_params=params(4),
        name="gram",
    )(*basis)
    parts = lax.all_to_all(jnp.broadcast_to(gram, (slabs, width)), "gx", 0, 0, tiled=True)
    return pl.pallas_call(
        functools.partial(output_kernel, start=start),
        out_shape=(shape(3, atoms), shape(3, atoms)),
        in_specs=[VMEM] * (ITERS + 3),
        out_specs=(VMEM, VMEM),
        scratch_shapes=[pltpu.VMEM((2 * rows, width), F32)],
        compiler_params=params(4),
        name="outputs",
    )(parts, inverse, *basis)


def solution(mesh):
    return jax.shard_map(
        on_device,
        mesh=mesh,
        in_specs=(
            P(None, REP_GX),
            P(REP_GX),
            P(None, REP_GX),
            P(REP_GX),
            P(REP_GX, None),
            P(None, REP_GX, None),
        ),
        out_specs=(P(None, REP_GX), P(None, REP_GX)),
        check_vma=False,
    )
```

```python
import functools

import jax
import jax.numpy as jnp
from jax import lax
from jax.experimental import pallas as pl
from jax.experimental.pallas import tpu as pltpu
from jax.sharding import PartitionSpec as P

ITERS = 4
REP_GX = ("rep", "gx")
THOLE = 0.39
SHIFT = 2.5
SCALE = 1.5
MATS = 4
OUT_SLOTS = 8
SLOTS = 10
MIB = 2**20

F32 = jnp.float32
VMEM = pl.BlockSpec(memory_space=pltpu.VMEM)
SMEM = pl.BlockSpec(memory_space=pltpu.SMEM)
HBM = pl.BlockSpec(memory_space=pltpu.MemorySpace.HBM)


def spread(row, height=8):
    return jnp.broadcast_to(row, (height, row.shape[1]))


def lane_pick(row_block, lanes):
    return jnp.take_along_axis(row_block, lanes, axis=1)


def params(mib):
    return pltpu.CompilerParams(vmem_limit_bytes=mib * MIB)


def tile_in_kernel(pos_hbm, pol_hbm, fld_hbm, idx_hbm, out_ref, pos_ref, pol_ref, fld_ref, idx_ref, sems):
    copies = [
        pltpu.make_async_copy(source, target, sems.at[k])
        for k, (source, target) in enumerate(
            ((idx_hbm, idx_ref), (pos_hbm, pos_ref), (pol_hbm, pol_ref), (fld_hbm, fld_ref))
        )
    ]
    for copy in copies:
        copy.start()
    for copy in copies:
        copy.wait()
    tiles, width = idx_ref.shape
    for q in range(tiles // 8):
        rows = idx_ref[8 * q : 8 * q + 8, :]
        high = rows // width
        low = rows - high * width

        def step(h, acc):
            at = pl.ds(pl.multiple_of(h * width, width), width)
            hit = high == h
            new = []
            for c in range(7):
                if c < 3:
                    row = pos_ref[c : c + 1, at]
                elif c == 3:
                    row = pol_ref[0:1, at]
                else:
                    row = fld_ref[c - 4 : c - 3, at]
                new.append(jnp.where(hit, lane_pick(spread(row), low), acc[c]))
            return tuple(new)

        acc = lax.fori_loop(0, tiles, step, (jnp.zeros((8, width), F32),) * 7, unroll=16)
        values = list(acc[:3]) + [lax.rsqrt(acc[3])] + list(acc[4:]) + [1.0 / acc[3]]
        for c in range(8):
            out_ref[c * tiles + 8 * q : c * tiles + 8 * q + 8, :] = values[c]


def inverse_kernel(idx_ref, out_ref):
    tiles, width = idx_ref.shape
    total = jnp.zeros((2 * tiles, width), F32)
    lane = lax.broadcasted_iota(jnp.int32, (tiles, width), 1).astype(F32)
    row_id = lax.broadcasted_iota(jnp.int32, (tiles, width), 0)
    low_id = lax.broadcasted_iota(jnp.int32, (width, width), 0)
    for t in range(tiles):
        row = idx_ref[t : t + 1, :]
        high = row // width
        low = row - high * width
        hit = spread(high, tiles) == row_id
        left = jnp.concatenate([jnp.where(hit, float(t), 0.0), jnp.where(hit, lane, 0.0)], axis=0)
        right = jnp.where(spread(low, width) == low_id, 1.0, 0.0)
        total = total + lax.dot_general(
            left.astype(jnp.bfloat16),
            right.astype(jnp.bfloat16),
            (((1,), (1,)), ((), ())),
            preferred_element_type=F32,
        )
    out_ref[...] = (total[:tiles] * float(width) + total[tiles:] + 0.5).astype(jnp.int32)


def take_neighbours(par, near_ref, far_ref, nb_ref, start, rows):
    nb_ref[pl.ds(pl.multiple_of(par * rows, 8), rows), :] = near_ref[start : start + rows, :]
    nb_ref[pl.ds(pl.multiple_of((1 - par) * rows, 8), rows), :] = far_ref[start : start + rows, :]


def pair_coefficients(off, ci, rj, same):
    dist_sq = off[0] * off[0] + off[1] * off[1] + off[2] * off[2]
    if same is not None:
        dist_sq = jnp.where(same, 1.0, dist_sq)
    inv = lax.rsqrt(dist_sq)
    damp = (dist_sq * (dist_sq * inv)) * (ci * rj)
    decay = jnp.exp(-damp)
    inv_sq = inv * inv
    cube = inv_sq * inv
    g3 = (1.0 - decay) * cube
    g5 = (3.0 - (3.0 + 3.0 * damp) * decay) * (cube * inv_sq)
    root = g5 * lax.rsqrt(g5)
    if same is not None:
        g3 = jnp.where(same, 0.0, g3)
        root = jnp.where(same, 0.0, root)
    return [root * off[0], root * off[1], root * off[2], g3]


def pack_job(t, n, slot, y, z, spare=0):
    return t + n * 256 + slot * 65536 + (y + 2 * z + 4 * spare) * 16777216


def read_job(tab_ref, group, at, tiles):
    word = tab_ref[1 + group, at]
    t = word & 255
    last = word >> 24
    return t, (word >> 8) & 255, (word >> 16) & 255, t + (last >> 2) * tiles, last & 1, (last >> 1) & 1


def row_block(ref, first, tiles, n, count):
    return [spread(ref[pl.ds(first + c * tiles + n, 1), :]) for c in range(count)]


def write_columns(col_ref, place, own_ref, tiles, t):
    width = own_ref.shape[1]
    for c in range(4):
        row = own_ref[pl.ds(c * tiles + t, 1), :]
        if c == 3:
            row = row * THOLE
        first = (place * 4 + c) * width
        col_ref[first : first + width, :] = spread(row, width).T


def pair_block(col_ref, place, row, store, same, lead):
    width = col_ref.shape[1]
    for k in range(width // 8):
        first = place * 4 * width + 8 * k
        col = [col_ref[first + c * width : first + c * width + 8, :] for c in range(4)]
        if lead is not None:
            off = [(col[c] + lead[c]) - row[c] for c in range(3)]
        else:
            off = [row[c] - col[c] for c in range(3)]
        mask = None
        if same:
            i = lax.broadcasted_iota(jnp.int32, (8, width), 0) + 8 * k
            j = lax.broadcasted_iota(jnp.int32, (8, width), 1)
            mask = i == j
        store(k, pair_coefficients(off, col[3], row[3], mask))


def store_at(ref, base):
    width = ref.shape[1]

    def store(k, mats):
        for m in range(MATS):
            ref[pl.ds(base + m * width + 8 * k, 8), :] = mats[m]

    return store


def halves(count):
    return (count + 1) // 2


def local_pairs_kernel(own_list, own_shift, own_ref, tensor_ref, tab_ref, col_ref, *, boxes):
    tiles = own_ref.shape[0] // 8
    width = own_ref.shape[1]
    extra = own_list.shape[0] - 1
    cap = extra * tiles
    size = MATS * width

    def sort(k, counts):
        inner, outer = counts
        e = k // tiles
        t = k - e * tiles
        n = own_list[1 + e, t]
        y = own_shift[1 + e, 0, t]
        z = own_shift[1 + e, 1, t]
        near = (n < tiles).astype(jnp.int32)
        tab_ref[1, inner] = pack_job(t, n, tiles + k, y, z)
        tab_ref[2, outer] = pack_job(t, n - tiles * (1 - near), tiles + k, y, z)
        return inner + near, outer + 1 - near

    inner, outer = lax.fori_loop(0, cap, sort, (jnp.int32(0), jnp.int32(0)), unroll=8)
    tab_ref[1, inner] = pack_job(0, 0, tiles + cap, 1, 1, 1)
    tab_ref[2, outer] = pack_job(0, 0, tiles + cap, 1, 1, 1)
    tab_ref[0, 0] = inner
    tab_ref[0, 1] = outer

    def self_job(i, _):
        for p in range(2):
            t = 2 * i + p
            write_columns(col_ref, p, own_ref, tiles, t)
            store = store_at(tensor_ref, pl.multiple_of(t * size, size))
            pair_block(col_ref, p, row_block(own_ref, 0, tiles, t, 4), store, True, None)
        return 0

    lax.fori_loop(0, tiles // 2, self_job, 0)

    def inner_job(i, _):
        for p in range(2):
            t, n, slot, _tw, y, z = read_job(tab_ref, 0, 2 * i + p, tiles)
            write_columns(col_ref, p, own_ref, tiles, t)
            row = row_block(own_ref, 0, tiles, n, 4)
            row = [row[0], row[1] + y.astype(F32) * boxes[1], row[2] + z.astype(F32) * boxes[2], row[3]]
            pair_block(col_ref, p, row, store_at(tensor_ref, pl.multiple_of(slot * size, size)), False, None)
        return 0

    lax.fori_loop(0, halves(inner), inner_job, 0)


def cross_pairs_kernel(
    par_ref, own_tab, prev_list, prev_shift, own_ref, near_ref, far_ref, tensor_in,
    tensor_ref, prev_hbm, tab_ref, nb_ref, col_ref, out_slots, sems,
    *, boxes,
):
    del tensor_in
    tiles = own_ref.shape[0] // 8
    width = own_ref.shape[1]
    extra = prev_list.shape[0] - 1
    cap = extra * tiles
    size = MATS * width
    rows = 4 * tiles
    par = par_ref[0]
    wrap_next = par_ref[1].astype(F32) * boxes[0]
    wrap_prev = par_ref[2].astype(F32) * boxes[0]
    take_neighbours(par, near_ref, far_ref, nb_ref, 0, rows)

    def sort(k, count):
        e = k // tiles
        t = k - e * tiles
        n = prev_list[1 + e, t]
        own = jnp.maximum(n - tiles, 0)
        tab_ref[1, count] = pack_job(own, t, 0, prev_shift[1 + e, 0, t], prev_shift[1 + e, 1, t])
        return count + (n >= tiles).astype(jnp.int32)

    behind = lax.fori_loop(0, cap, sort, jnp.int32(0), unroll=8)
    tab_ref[1, behind] = pack_job(0, 0, 0, 0, 0, 1)
    tab_ref[0, 0] = behind
    outer = own_tab[0, 1]

    def out_copy(i):
        slot = lax.rem(i, OUT_SLOTS)
        return pltpu.make_async_copy(
            out_slots.at[pl.ds(pl.multiple_of(slot * size, size), size), :],
            prev_hbm.at[pl.ds(pl.multiple_of(i * size, size), size), :],
            sems.at[slot],
        )

    def behind_job(i, _):
        jobs = [read_job(tab_ref, 0, 2 * i + p, tiles) for p in range(2)]
        for p in range(2):

            @pl.when(2 * i + p >= OUT_SLOTS)
            def _():
                out_copy(2 * i + p - OUT_SLOTS).wait()

        for p in range(2):
            t, n, _slot, _tw, y, z = jobs[p]
            write_columns(col_ref, p, own_ref, tiles, t)
            lead = (wrap_prev, y.astype(F32) * boxes[1], z.astype(F32) * boxes[2])
            base = pl.multiple_of(lax.rem(2 * i + p, OUT_SLOTS) * size, size)
            pair_block(col_ref, p, row_block(nb_ref, rows, tiles, n, 4), store_at(out_slots, base), False, lead)
        for p in range(2):
            out_copy(2 * i + p).start()
        return 0

    steps = halves(behind)
    lax.fori_loop(0, steps, behind_job, 0)

    def outer_job(i, _):
        for p in range(2):
            t, n, slot, _tw, y, z = read_job(own_tab, 1, 2 * i + p, tiles)
            write_columns(col_ref, p, own_ref, tiles, t)
            row = row_block(nb_ref, 0, tiles, n, 4)
            row = [
                row[0] + wrap_next, row[1] + y.astype(F32) * boxes[1], row[2] + z.astype(F32) * boxes[2], row[3]
            ]
            pair_block(col_ref, p, row, store_at(tensor_ref, pl.multiple_of(slot * size, size)), False, None)
        return 0

    lax.fori_loop(0, halves(outer), outer_job, 0)

    def drain(i, _):
        out_copy(i).wait()
        return 0

    lax.fori_loop(jnp.maximum(2 * steps - OUT_SLOTS, 0), 2 * steps, drain, 0)


def left_at(tile, c, k, width):
    return pl.ds(pl.multiple_of((tile * 3 + c) * width, width) + 8 * k, 8)


def one_side(left_ref, source, base, tile, row, fresh):
    width = source.shape[1]
    for k in range(width // 8):
        s = [source[pl.ds(base + m * width + 8 * k, 8), :] for m in range(MATS)]
        lift = s[0] * row[0] + s[1] * row[1] + s[2] * row[2]
        for c in range(3):
            at = left_at(tile, c, k, width)
            value = s[c] * lift - s[3] * row[c]
            left_ref[at, :] = value if fresh else left_ref[at, :] + value


def lane_total(left_ref, t, c, width):
    block = left_ref[pl.ds(pl.multiple_of((t * 3 + c) * width, width), width), :].T
    return jnp.sum(block, axis=0, keepdims=True)


def local_apply_kernel(tab_ref, tensor_ref, own_ref, out_ref, left_ref, right_ref, *, start):
    width = own_ref.shape[1]
    rows = out_ref.shape[0]
    tiles = rows // 3
    size = MATS * width
    right_ref[...] = jnp.zeros_like(right_ref)

    def self_job(i, _):
        for p in range(2):
            t = 2 * i + p
            row = row_block(own_ref, start, tiles, t, 3)
            one_side(left_ref, tensor_ref, pl.multiple_of(t * size, size), t, row, True)
        return 0

    lax.fori_loop(0, tiles // 2, self_job, 0)
    first = pl.multiple_of(tiles * 3 * width, width)
    left_ref[pl.ds(first, 3 * width), :] = jnp.zeros((3 * width, width), F32)

    def inner_job(i, _):
        jobs = [read_job(tab_ref, 0, 2 * i + p, tiles)[:4] for p in range(2)]
        cols = [
            [spread(own_ref[pl.ds(start + c * tiles + job[0], 1), :], width).T for c in range(3)] for job in jobs
        ]
        for (t, n, slot, tw), col in zip(jobs, cols):
            row = row_block(own_ref, start, tiles, n, 3)
            one_side(left_ref, tensor_ref, pl.multiple_of(slot * size, size), tw, row, False)
        for (t, n, slot, tw), col in zip(jobs, cols):
            base = pl.multiple_of(slot * size, size)
            target = jnp.where(tw < tiles, n, tiles)
            places = [pl.ds(pl.multiple_of((target * 3 + c) * 8, 8), 8) for c in range(3)]
            acc = [jnp.zeros((8, width), F32)] * 3
            for q in range(width // 8):
                s = [tensor_ref[pl.ds(base + m * width + 8 * q, 8), :] for m in range(MATS)]
                mine = [col[c][8 * q : 8 * q + 8, :] for c in range(3)]
                lift = s[0] * mine[0] + s[1] * mine[1] + s[2] * mine[2]
                for c in range(3):
                    acc[c] = acc[c] + (s[c] * lift - s[3] * mine[c])
            for c in range(3):
                right_ref[places[c], :] = right_ref[places[c], :] + acc[c]
        return 0

    lax.fori_loop(0, halves(tab_ref[0, 0]), inner_job, 0)

    def finish(t, _):
        for c in range(3):
            field = lane_total(left_ref, t, c, width) + jnp.sum(
                right_ref[pl.ds(pl.multiple_of((t * 3 + c) * 8, 8), 8), :], axis=0, keepdims=True
            )
            out_ref[pl.ds(c * tiles + t, 1), :] = field
        return 0

    lax.fori_loop(0, tiles, finish, 0, unroll=4)


def cross_apply_kernel(
    par_ref, own_tab, prev_tab, tensor_ref, prev_hbm, own_ref, near_ref, far_ref, inv_ref, part_ref,
    out_ref, nb_ref, left_ref, slots_ref, sems,
    *, start, inv_start,
):
    width = own_ref.shape[1]
    rows = out_ref.shape[0]
    tiles = rows // 3
    size = MATS * width
    behind = prev_tab[0, 0]

    def in_copy(i):
        slot = lax.rem(i, SLOTS)
        return pltpu.make_async_copy(
            prev_hbm.at[pl.ds(pl.multiple_of(i * size, size), size), :],
            slots_ref.at[pl.ds(pl.multiple_of(slot * size, size), size), :],
            sems.at[slot],
        )

    steps = halves(behind)

    def begin(i, _):
        in_copy(i).start()
        return 0

    lax.fori_loop(0, jnp.minimum(2 * steps, SLOTS), begin, 0)
    take_neighbours(par_ref[0], near_ref, far_ref, nb_ref, start, rows)

    def clear(i, _):
        left_ref[pl.ds(pl.multiple_of(i * width, width), width), :] = jnp.zeros((width, width), F32)
        return 0

    lax.fori_loop(0, rows + 3, clear, 0, unroll=3)

    def outer_job(i, _):
        for p in range(2):
            t, n, slot, tw = read_job(own_tab, 1, 2 * i + p, tiles)[:4]
            row = row_block(nb_ref, 0, tiles, n, 3)
            one_side(left_ref, tensor_ref, pl.multiple_of(slot * size, size), tw, row, False)
        return 0

    lax.fori_loop(0, halves(own_tab[0, 1]), outer_job, 0)

    def behind_job(i, _):
        jobs = [read_job(prev_tab, 0, 2 * i + p, tiles)[:4] for p in range(2)]
        for p in range(2):
            in_copy(2 * i + p).wait()
        for p in range(2):
            t, n, slot, tw = jobs[p]
            base = pl.multiple_of(lax.rem(2 * i + p, SLOTS) * size, size)
            one_side(left_ref, slots_ref, base, tw, row_block(nb_ref, rows, tiles, n, 3), False)

        @pl.when(2 * i + SLOTS < 2 * steps)
        def _():
            for p in range(2):
                in_copy(2 * i + p + SLOTS).start()

        return 0

    lax.fori_loop(0, steps, behind_job, 0)

    def finish(t, _):
        weight = (inv_ref[pl.ds(inv_start + t, 1), :] - SHIFT) * (1.0 / SCALE)
        for c in range(3):
            at = pl.ds(c * tiles + t, 1)
            field = lane_total(left_ref, t, c, width) + part_ref[at, :]
            mine = own_ref[pl.ds(start + c * tiles + t, 1), :]
            out_ref[at, :] = mine * weight - field * (1.0 / SCALE)
        return 0

    lax.fori_loop(0, tiles, finish, 0, unroll=4)


PAIRS = [(i, j) for i in range(ITERS + 1) for j in range(i, ITERS + 1)]


def gram_kernel(*refs, start):
    vectors, out_ref = refs[:-1], refs[-1]
    rows, width = vectors[-1].shape
    lane = lax.broadcasted_iota(jnp.int32, (1, width), 1)
    total = jnp.zeros((1, width), F32)
    starts = (start,) + (0,) * ITERS
    for n, (i, j) in enumerate(PAIRS):
        product = vectors[i][starts[i] : starts[i] + rows, :] * vectors[j][starts[j] : starts[j] + rows, :]
        line = jnp.sum(product, axis=0, keepdims=True)
        total = jnp.where(lane == n, jnp.sum(line, axis=1, keepdims=True), total)
    out_ref[...] = total


def untile_kernel(inv_ref, *refs, start):
    vectors, outs = refs[: ITERS + 1], refs[ITERS + 1 :]
    tiles, width = inv_ref.shape
    starts = (start,) + (0,) * ITERS
    zero = jnp.zeros((8, width), F32)
    for q in range(tiles // 8):
        index = inv_ref[8 * q : 8 * q + 8, :]
        high = index // width
        low = index - high * width

        def step(h, acc):
            hit = high == h
            return tuple(
                jnp.where(hit, lane_pick(spread(vectors[n // 3][pl.ds(starts[n // 3] + n % 3 * tiles + h, 1), :]), low), acc[n])
                for n in range(3 * (ITERS + 1))
            )

        acc = lax.fori_loop(0, tiles, step, (zero,) * (3 * (ITERS + 1)), unroll=8)
        for n in range(3 * (ITERS + 1)):
            for s in range(8):
                at = (8 * q + s) * width
                outs[n // 3][n % 3 : n % 3 + 1, at : at + width] = acc[n][s : s + 1, :]


def output_kernel(parts_ref, *refs):
    vectors, (dip_ref, res_ref) = refs[: ITERS + 1], refs[ITERS + 1 :]
    width = parts_ref.shape[1]
    sums = jnp.sum(parts_ref[...], axis=0, keepdims=True)
    lane = lax.broadcasted_iota(jnp.int32, (1, width), 1)
    gram = {}
    for n, (i, j) in enumerate(PAIRS):
        value = jnp.sum(jnp.where(lane == n, sums, 0.0), axis=1, keepdims=True)
        gram[i, j] = gram[j, i] = jnp.broadcast_to(value, (1, width))

    def add(a, b):
        return b if a is None else a if b is None else a + b

    def inner(a, b):
        total = None
        for i in range(ITERS + 1):
            line = None
            for j in range(ITERS + 1):
                if a[i] is not None and b[j] is not None:
                    line = add(line, b[j] * gram[i, j])
            if line is not None:
                total = add(total, a[i] * line)
        return total

    def operate(a):
        out = [None if v is None else SHIFT * v for v in a]
        for i in range(ITERS):
            if a[i] is not None:
                out[i + 1] = add(out[i + 1], SCALE * a[i])
        return out

    x = [None] * (ITERS + 1)
    r = [jnp.ones((1, width), F32)] + [None] * ITERS
    d = list(r)
    norm = inner(r, r)
    for step in range(ITERS):
        q = operate(d)
        size = norm / inner(d, q)
        x = [add(x[k], None if d[k] is None else size * d[k]) for k in range(ITERS + 1)]
        r = [add(r[k], None if q[k] is None else -size * q[k]) for k in range(ITERS + 1)]
        if step + 1 < ITERS:
            new = inner(r, r)
            ratio = new / norm
            d = [add(r[k], None if d[k] is None else ratio * d[k]) for k in range(ITERS + 1)]
            norm = new
    x = [None if v is None else jnp.broadcast_to(v, (3, width)) for v in x]
    r = [jnp.broadcast_to(v, (3, width)) for v in r]
    for b in range(dip_ref.shape[1] // width):
        at = slice(b * width, (b + 1) * width)
        values = [vectors[k][:, at] for k in range(ITERS + 1)]
        for out, weights in ((dip_ref, x), (res_ref, r)):
            total = None
            for k in range(ITERS + 1):
                if weights[k] is not None:
                    total = add(total, weights[k] * values[k])
            out[:, at] = total


def shape(rows, width, dtype=F32):
    return jax.ShapeDtypeStruct((rows, width), dtype)


def cost(flops):
    return pl.CostEstimate(flops=flops, bytes_accessed=1_000_000, transcendentals=0)


def on_device(positions, polar, field_ext, tile_atom, tile_list, image_shift):
    tiles, links = tile_list.shape
    atoms = tile_atom.shape[0]
    width = atoms // tiles
    slabs = lax.axis_size("gx")
    slab = lax.axis_index("gx")
    rows = 3 * tiles
    cap = tiles * (links - 1)
    size = MATS * width
    boxes = (4.0 * slabs, 128.0, 2.0 * tiles)
    near_pairs = [(i, i ^ 1) for i in range(slabs)]
    far_pairs = [(i, ((i + 1) ^ 1) - 1 if 0 < i < slabs - 1 else slabs - 1 - i) for i in range(slabs)]
    ahead = [(i, (i + 1) % slabs) for i in range(slabs)]

    def swap(value):
        return lax.ppermute(value, "gx", far_pairs), lax.ppermute(value, "gx", near_pairs)

    own_list = tile_list.T
    own_shift = image_shift.transpose(2, 0, 1)
    prev_list = lax.ppermute(own_list, "gx", ahead)
    prev_shift = lax.ppermute(own_shift, "gx", ahead)
    par = jnp.stack([slab % 2, (slab == slabs - 1).astype(jnp.int32), (slab == 0).astype(jnp.int32)])
    par = par.astype(jnp.int32)
    index = tile_atom.reshape(tiles, width)
    packed = pl.pallas_call(
        tile_in_kernel,
        out_shape=shape(8 * tiles, width),
        in_specs=[HBM] * 4,
        out_specs=VMEM,
        scratch_shapes=[
            pltpu.VMEM((3, atoms), F32),
            pltpu.VMEM((1, atoms), F32),
            pltpu.VMEM((3, atoms), F32),
            pltpu.VMEM((tiles, width), jnp.int32),
            pltpu.SemaphoreType.DMA((4,)),
        ],
        compiler_params=params(4),
        name="tile_in",
    )(*(pltpu.with_memory_space_constraint(v, pltpu.MemorySpace.HBM) for v in (positions, polar.reshape(1, -1), field_ext, index)))
    far, near = swap(packed)
    inverse = pl.pallas_call(
        inverse_kernel,
        out_shape=shape(tiles, width, jnp.int32),
        in_specs=[VMEM],
        out_specs=VMEM,
        compiler_params=params(4),
        cost_estimate=cost(4_000_000),
        name="inverse",
    )(index)
    table = shape(3, cap + 1, jnp.int32)
    tensor_shape = pltpu.VMEM(((tiles + cap + 1) * size, width), F32)
    col_shape = pltpu.VMEM((2 * 4 * width, width), F32)
    tensor, own_tab = pl.pallas_call(
        functools.partial(local_pairs_kernel, boxes=boxes),
        out_shape=(tensor_shape, table),
        in_specs=[SMEM, SMEM, VMEM],
        out_specs=(VMEM, SMEM),
        scratch_shapes=[col_shape],
        compiler_params=params(4),
        cost_estimate=cost(60_000_000),
        name="local_pairs",
    )(own_list, own_shift, packed)
    tensor, prev_tensor, prev_tab = pl.pallas_call(
        functools.partial(cross_pairs_kernel, boxes=boxes),
        out_shape=(
            tensor_shape,
            pltpu.MemorySpace.HBM(((cap + 1) * size, width), F32),
            table,
        ),
        in_specs=[SMEM] * 4 + [VMEM] * 4,
        out_specs=(VMEM, HBM, SMEM),
        scratch_shapes=[
            pltpu.VMEM((2 * 4 * tiles, width), F32),
            col_shape,
            pltpu.VMEM((OUT_SLOTS * size, width), F32),
            pltpu.SemaphoreType.DMA((OUT_SLOTS,)),
        ],
        input_output_aliases={7: 0},
        compiler_params=params(6),
        cost_estimate=cost(60_000_000),
        name="cross_pairs",
    )(par, own_tab, prev_list, prev_shift, packed, near, far, tensor)
    prev_tensor = pltpu.with_memory_space_constraint(prev_tensor, pltpu.MemorySpace.HBM)
    left_shape = pltpu.VMEM(((rows + 3) * width, width), F32)

    def apply(vector, near, far, start):
        part = pl.pallas_call(
            functools.partial(local_apply_kernel, start=start),
            out_shape=shape(rows, width),
            in_specs=[SMEM, VMEM, VMEM],
            out_specs=VMEM,
            scratch_shapes=[left_shape, pltpu.VMEM((8 * (rows + 3), width), F32)],
            compiler_params=params(9),
            cost_estimate=cost(60_000_000),
            name="local_apply",
        )(own_tab, tensor, vector)
        return pl.pallas_call(
            functools.partial(cross_apply_kernel, start=start, inv_start=7 * tiles),
            out_shape=shape(rows, width),
            in_specs=[SMEM] * 3 + [VMEM, HBM] + [VMEM] * 5,
            out_specs=VMEM,
            scratch_shapes=[
                pltpu.VMEM((2 * rows, width), F32),
                left_shape,
                pltpu.VMEM((SLOTS * size, width), F32),
                pltpu.SemaphoreType.DMA((SLOTS,)),
            ],
            compiler_params=params(10),
            cost_estimate=cost(60_000_000),
            name="cross_apply",
        )(par, own_tab, prev_tab, tensor, prev_tensor, vector, near, far, packed, part)

    start = 4 * tiles
    basis = [packed]
    vector = apply(packed, near, far, start)
    basis.append(vector)
    for _ in range(ITERS - 1):
        far, near = swap(vector)
        vector = apply(vector, near, far, 0)
        basis.append(vector)
    gram = pl.pallas_call(
        functools.partial(gram_kernel, start=start),
        out_shape=shape(1, width),
        in_specs=[VMEM] * (ITERS + 1),
        out_specs=VMEM,
        compiler_params=params(4),
        name="gram",
    )(*basis)
    parts = lax.all_to_all(jnp.broadcast_to(gram, (slabs, width)), "gx", 0, 0, tiled=True)
    natural = pl.pallas_call(
        functools.partial(untile_kernel, start=start),
        out_shape=(shape(3, atoms),) * (ITERS + 1),
        in_specs=[VMEM] * (ITERS + 2),
        out_specs=(VMEM,) * (ITERS + 1),
        compiler_params=params(4),
        cost_estimate=cost(60_000_000),
        name="untile",
    )(inverse, *basis)
    return pl.pallas_call(
        output_kernel,
        out_shape=(shape(3, atoms), shape(3, atoms)),
        in_specs=[VMEM] * (ITERS + 2),
        out_specs=(VMEM, VMEM),
        compiler_params=params(4),
        name="outputs",
    )(parts, *natural)


def solution(mesh):
    return jax.shard_map(
        on_device,
        mesh=mesh,
        in_specs=(
            P(None, REP_GX),
            P(REP_GX),
            P(None, REP_GX),
            P(REP_GX),
            P(REP_GX, None),
            P(None, REP_GX, None),
        ),
        out_specs=(P(None, REP_GX), P(None, REP_GX)),
        check_vma=False,
    )
```

```python
import functools

import jax
import jax.numpy as jnp
from jax import lax
from jax.experimental import pallas as pl
from jax.experimental.pallas import tpu as pltpu
from jax.sharding import PartitionSpec as P

ITERS = 4
REP_GX = ("rep", "gx")
THOLE = 0.39
SHIFT = 2.5
SCALE = 1.5
MATS = 4
OUT_SLOTS = 12
BATCH = 8
HALF = 4
PAD = 12
GROUP = 16
SLOTS = 24
MIB = 2**20

F32 = jnp.float32
VMEM = pl.BlockSpec(memory_space=pltpu.VMEM)
SMEM = pl.BlockSpec(memory_space=pltpu.SMEM)
HBM = pl.BlockSpec(memory_space=pltpu.MemorySpace.HBM)


def spread(row, height=8):
    return jnp.broadcast_to(row, (height, row.shape[1]))


def lane_pick(row_block, lanes):
    return jnp.take_along_axis(row_block, lanes, axis=1)


def params(mib):
    return pltpu.CompilerParams(vmem_limit_bytes=mib * MIB)


def tile_in_kernel(pos_hbm, pol_hbm, fld_hbm, idx_hbm, out_ref, pos_ref, pol_ref, fld_ref, idx_ref, sems):
    copies = [
        pltpu.make_async_copy(source, target, sems.at[k])
        for k, (source, target) in enumerate(
            ((idx_hbm, idx_ref), (pos_hbm, pos_ref), (pol_hbm, pol_ref), (fld_hbm, fld_ref))
        )
    ]
    for copy in copies:
        copy.start()
    for copy in copies:
        copy.wait()
    tiles, width = idx_ref.shape
    for q in range(tiles // 8):
        rows = idx_ref[8 * q : 8 * q + 8, :]
        high = rows // width
        low = rows - high * width

        def step(h, acc):
            at = pl.ds(pl.multiple_of(h * width, width), width)
            hit = high == h
            new = []
            for c in range(7):
                if c < 3:
                    row = pos_ref[c : c + 1, at]
                elif c == 3:
                    row = pol_ref[0:1, at]
                else:
                    row = fld_ref[c - 4 : c - 3, at]
                new.append(jnp.where(hit, lane_pick(spread(row), low), acc[c]))
            return tuple(new)

        acc = lax.fori_loop(0, tiles, step, (jnp.zeros((8, width), F32),) * 7, unroll=16)
        values = list(acc[:3]) + [lax.rsqrt(acc[3])] + list(acc[4:]) + [1.0 / acc[3]]
        for c in range(8):
            out_ref[c * tiles + 8 * q : c * tiles + 8 * q + 8, :] = values[c]


def inverse_kernel(idx_ref, out_ref):
    tiles, width = idx_ref.shape
    total = jnp.zeros((2 * tiles, width), F32)
    lane = lax.broadcasted_iota(jnp.int32, (tiles, width), 1).astype(F32)
    row_id = lax.broadcasted_iota(jnp.int32, (tiles, width), 0)
    low_id = lax.broadcasted_iota(jnp.int32, (width, width), 0)
    for t in range(tiles):
        row = idx_ref[t : t + 1, :]
        high = row // width
        low = row - high * width
        hit = spread(high, tiles) == row_id
        left = jnp.concatenate([jnp.where(hit, float(t), 0.0), jnp.where(hit, lane, 0.0)], axis=0)
        right = jnp.where(spread(low, width) == low_id, 1.0, 0.0)
        total = total + lax.dot_general(
            left.astype(jnp.bfloat16),
            right.astype(jnp.bfloat16),
            (((1,), (1,)), ((), ())),
            preferred_element_type=F32,
        )
    out_ref[...] = (total[:tiles] * float(width) + total[tiles:] + 0.5).astype(jnp.int32)


def pair_coefficients(off, ri, rj, same):
    dist_sq = off[0] * off[0] + off[1] * off[1] + off[2] * off[2]
    if same is not None:
        dist_sq = jnp.where(same, 1.0, dist_sq)
    inv = lax.rsqrt(dist_sq)
    damp = (dist_sq * (dist_sq * inv)) * (THOLE * ri * rj)
    decay = jnp.exp(-damp)
    inv_sq = inv * inv
    cube = inv_sq * inv
    g3 = (1.0 - decay) * cube
    g5 = (3.0 - (3.0 + 3.0 * damp) * decay) * (cube * inv_sq)
    root = g5 * lax.rsqrt(g5)
    if same is not None:
        g3 = jnp.where(same, 0.0, g3)
        root = jnp.where(same, 0.0, root)
    return [root * off[0], root * off[1], root * off[2], g3]


def split_rows(a_ref, first_tile, ref, first, tiles, comps):
    for c in range(comps):
        rest = ref[first + c * tiles : first + (c + 1) * tiles, :]
        for k in range(3):
            part = rest.astype(jnp.bfloat16).astype(F32) if k < 2 else rest
            a_ref[pl.ds(first_tile * GROUP + 3 * c + k, tiles, stride=GROUP), :] = part
            rest = rest - part


def selector(comps, width):
    k = lax.broadcasted_iota(jnp.int32, (GROUP, comps * width), 0)
    lane = lax.broadcasted_iota(jnp.int32, (GROUP, comps * width), 1)
    first = lane // width * 3
    return jnp.where(jnp.logical_and(k >= first, k < first + 3), 1.0, 0.0).astype(jnp.bfloat16)


def turn_rows(at_ref, a_ref):
    width = a_ref.shape[1]

    def turn(t, _):
        part = a_ref[pl.ds(pl.multiple_of(t * GROUP, GROUP), GROUP), :].astype(jnp.bfloat16)
        at_ref[pl.ds(pl.multiple_of(t * width, width), width), :] = part.T
        return 0

    lax.fori_loop(0, a_ref.shape[0] // GROUP, turn, 0, unroll=8)


def write_columns(col_ref, place, at_ref, tile, select):
    width = col_ref.shape[0] // HALF
    part = at_ref[pl.ds(pl.multiple_of(tile * width, width), width), :]
    col_ref[place * width : (place + 1) * width, :] = jnp.dot(part, select, preferred_element_type=F32)


def pipelined(count, columns, compute, cols, before=None, after=None):
    first, second = cols
    columns(0, first)

    def body(i, _):
        if before is not None:
            before(i)
        columns(2 * i + 1, second)
        compute(2 * i, first, 0)
        columns(2 * i + 2, first)
        compute(2 * i + 1, second, 1)
        if after is not None:
            after(i)
        return 0

    lax.fori_loop(0, (count + BATCH - 1) // BATCH, body, 0)


def pack_job(t, n, slot, y, z, spare=0):
    return t + n * 256 + slot * 65536 + (y + 2 * z + 4 * spare) * 16777216


def pad_jobs(tab_ref, line, count, slot, y, z):
    for k in range(PAD):
        tab_ref[line, count + k] = pack_job(0, 0, slot, y, z, 1)


def target_source(word):
    return word & 255, (word >> 8) & 255


def row_block(ref, tiles, n, count):
    return [spread(ref[pl.ds(c * tiles + n, 1), :]) for c in range(count)]


def pair_block(col_ref, place, row, kind, lead, store):
    width = row[0].shape[1]
    if kind == "row":
        row = [row[c] + lead[c] for c in range(3)] + [row[3]]
    for k in range(width // 8):
        first = place * width + 8 * k
        col = [col_ref[first : first + 8, c * width : (c + 1) * width] for c in range(4)]
        if kind == "col":
            off = [(col[c] + lead[c]) - row[c] for c in range(3)]
        else:
            off = [row[c] - col[c] for c in range(3)]
        mask = None
        if kind == "self":
            i = lax.broadcasted_iota(jnp.int32, (8, width), 0) + 8 * k
            j = lax.broadcasted_iota(jnp.int32, (8, width), 1)
            mask = i == j
        store(k, pair_coefficients(off, col[3], row[3], mask))


def store_at(ref, base):
    width = ref.shape[1]

    def store(k, mats):
        for m in range(MATS):
            ref[pl.ds(base + m * width + 8 * k, 8), :] = mats[m]

    return store


def rounded(count):
    return (count + BATCH - 1) // BATCH * BATCH


class Stream:
    def __init__(self, hbm, slots, sems, size, depth, inward):
        self.parts = (hbm, slots, sems, size, depth, inward)

    def base(self, i):
        _, _, _, size, depth, _ = self.parts
        return pl.multiple_of(lax.rem(i, depth) * size, size)

    def copy(self, i):
        hbm, slots, sems, size, depth, inward = self.parts
        far = hbm.at[pl.ds(pl.multiple_of(i * size, size), size), :]
        near = slots.at[pl.ds(self.base(i), size), :]
        sem = sems.at[lax.rem(i, depth)]
        return pltpu.make_async_copy(far, near, sem) if inward else pltpu.make_async_copy(near, far, sem)

    def start(self, low, high):
        def one(i, _):
            self.copy(i).start()
            return 0

        lax.fori_loop(low, high, one, 0)

    def wait(self, low, high):
        def one(i, _):
            self.copy(i).wait()
            return 0

        lax.fori_loop(low, high, one, 0)


def make_pairs(tab_ref, line, count, at_ref, a_first, own_ref, cols, select, kind, boxes, wrap, target, stream=None):
    tiles = own_ref.shape[0] // 8
    width = own_ref.shape[1]
    size = MATS * width

    def columns(j, col_ref):
        for p in range(HALF):
            _, n = target_source(tab_ref[line, HALF * j + p])
            write_columns(col_ref, p, at_ref, a_first + n, select)

    def compute(j, col_ref, _half):
        for p in range(HALF):
            word = tab_ref[line, HALF * j + p]
            t, _ = target_source(word)
            last = word >> 24
            lead = (wrap, (last & 1).astype(F32) * boxes[1], ((last >> 1) & 1).astype(F32) * boxes[2])
            if stream is None:
                base = pl.multiple_of(((word >> 16) & 255) * size, size)
            else:
                base = stream.base(HALF * j + p)
            pair_block(col_ref, p, row_block(own_ref, tiles, t, 4), kind, lead, store_at(target, base))

    if stream is None:
        pipelined(count, columns, compute, cols)
        return
    depth = stream.parts[4]

    def before(i):
        for p in range(BATCH):

            @pl.when(BATCH * i + p >= depth)
            def _():
                stream.copy(BATCH * i + p - depth).wait()

    def after(i):
        for p in range(BATCH):
            stream.copy(BATCH * i + p).start()

    pipelined(count, columns, compute, cols, before, after)


def local_pairs_kernel(
    own_list, own_shift, own_ref, tensor_ref, back_hbm, tab_ref, a_ref, at_ref, col_a, col_b, slots, sems, *, boxes
):
    tiles = own_ref.shape[0] // 8
    width = own_ref.shape[1]
    extra = own_list.shape[0] - 1
    cap = extra * tiles
    size = MATS * width
    for t in range(tiles):
        tab_ref[1, t] = pack_job(t, t, t, 0, 0)

    def sort(k, counts):
        inner, outer = counts
        e = k // tiles
        t = k - e * tiles
        n = own_list[1 + e, t]
        y = own_shift[1 + e, 0, t]
        z = own_shift[1 + e, 1, t]
        near = (n < tiles).astype(jnp.int32)
        tab_ref[1, tiles + inner] = pack_job(n * near, t, tiles + k, y, z)
        tab_ref[2, outer] = pack_job(t, n - tiles * (1 - near), tiles + k, y, z)
        tab_ref[3, inner] = pack_job(t, n * near, 0, y, z)
        return inner + near, outer + 1 - near

    inner, outer = lax.fori_loop(0, cap, sort, (jnp.int32(0), jnp.int32(0)), unroll=8)
    pad_jobs(tab_ref, 1, tiles + inner, tiles + cap, 1, 1)
    pad_jobs(tab_ref, 2, outer, tiles + cap, 1, 1)
    pad_jobs(tab_ref, 3, inner, 0, 1, 1)
    tab_ref[0, 0] = inner
    tab_ref[0, 1] = outer
    a_ref[...] = jnp.zeros_like(a_ref)
    split_rows(a_ref, 0, own_ref, 0, tiles, 4)
    turn_rows(at_ref, a_ref)
    select = selector(4, width)
    cols = (col_a, col_b)
    make_pairs(tab_ref, 1, tiles, at_ref, 0, own_ref, cols, select, "self", boxes, 0.0, tensor_ref)
    stream = Stream(back_hbm, slots, sems, size, OUT_SLOTS, False)
    make_pairs(tab_ref, 3, inner, at_ref, 0, own_ref, cols, select, "col", boxes, 0.0, slots, stream)

    def shifted_columns(j, col_ref):
        for p in range(HALF):
            _, n = target_source(tab_ref[1, tiles + HALF * j + p])
            write_columns(col_ref, p, at_ref, n, select)

    def shifted_compute(j, col_ref, _half):
        for p in range(HALF):
            word = tab_ref[1, tiles + HALF * j + p]
            t, _ = target_source(word)
            last = word >> 24
            lead = (0.0, (last & 1).astype(F32) * boxes[1], ((last >> 1) & 1).astype(F32) * boxes[2])
            base = pl.multiple_of(((word >> 16) & 255) * size, size)
            pair_block(col_ref, p, row_block(own_ref, tiles, t, 4), "row", lead, store_at(tensor_ref, base))

    pipelined(inner, shifted_columns, shifted_compute, cols)
    done = rounded(inner)
    stream.wait(jnp.maximum(done - OUT_SLOTS, 0), done)


def cross_pairs_kernel(
    par_ref, own_tab, prev_list, prev_shift, own_ref, near_ref, far_ref, tensor_in,
    tensor_ref, prev_hbm, tab_ref, a_ref, at_ref, col_a, col_b, slots, sems,
    *, boxes,
):
    del tensor_in
    tiles = own_ref.shape[0] // 8
    width = own_ref.shape[1]
    extra = prev_list.shape[0] - 1
    cap = extra * tiles
    size = MATS * width
    par = par_ref[0]
    wrap_next = par_ref[1].astype(F32) * boxes[0]
    wrap_prev = par_ref[2].astype(F32) * boxes[0]
    a_ref[...] = jnp.zeros_like(a_ref)
    split_rows(a_ref, par * tiles, near_ref, 0, tiles, 4)
    split_rows(a_ref, (1 - par) * tiles, far_ref, 0, tiles, 4)

    def sort(k, count):
        e = k // tiles
        t = k - e * tiles
        n = prev_list[1 + e, t]
        own = jnp.maximum(n - tiles, 0)
        tab_ref[1, count] = pack_job(own, t, 0, prev_shift[1 + e, 0, t], prev_shift[1 + e, 1, t])
        return count + (n >= tiles).astype(jnp.int32)

    behind = lax.fori_loop(0, cap, sort, jnp.int32(0), unroll=8)
    pad_jobs(tab_ref, 1, behind, 0, 0, 0)
    tab_ref[0, 0] = behind
    turn_rows(at_ref, a_ref)
    select = selector(4, width)
    cols = (col_a, col_b)
    stream = Stream(prev_hbm, slots, sems, size, OUT_SLOTS, False)
    make_pairs(tab_ref, 1, behind, at_ref, tiles, own_ref, cols, select, "row", boxes, wrap_prev, slots, stream)
    make_pairs(own_tab, 2, own_tab[0, 1], at_ref, 0, own_ref, cols, select, "col", boxes, wrap_next, tensor_ref)
    done = rounded(behind)
    stream.wait(jnp.maximum(done - OUT_SLOTS, 0), done)


def apply_jobs(tab_ref, line, count, at_ref, a_first, cols, select, field_ref, source, stream=None):
    width = field_ref.shape[1]
    size = MATS * width
    tiles = field_ref.shape[0] // 24 - 1

    def columns(j, col_ref):
        for p in range(HALF):
            _, n = target_source(tab_ref[line, HALF * j + p])
            write_columns(col_ref, p, at_ref, a_first + n, select)

    def compute(j, col_ref, _half):
        for p in range(HALF):
            word = tab_ref[line, HALF * j + p]
            t, _ = target_source(word)
            t = t + ((word >> 26) & 1) * tiles
            if stream is None:
                base = pl.multiple_of(((word >> 16) & 255) * size, size)
            else:
                base = stream.base(HALF * j + p)
            acc = [jnp.zeros((8, width), F32)] * 3
            for q in range(width // 8):
                s = [source[pl.ds(base + m * width + 8 * q, 8), :] for m in range(MATS)]
                first = p * width + 8 * q
                mine = [col_ref[first : first + 8, c * width : (c + 1) * width] for c in range(3)]
                lift = s[0] * mine[0] + s[1] * mine[1] + s[2] * mine[2]
                for c in range(3):
                    acc[c] = acc[c] + (s[c] * lift - s[3] * mine[c])
            for c in range(3):
                at = pl.ds(pl.multiple_of((t * 3 + c) * 8, 8), 8)
                field_ref[at, :] = field_ref[at, :] + acc[c]

    if stream is None:
        pipelined(count, columns, compute, cols)
        return
    depth = stream.parts[4]
    total = rounded(count)

    def before(i):
        for p in range(BATCH):
            stream.copy(BATCH * i + p).wait()

    def after(i):
        @pl.when(BATCH * i + depth < total)
        def _():
            for p in range(BATCH):
                stream.copy(BATCH * i + p + depth).start()

    pipelined(count, columns, compute, cols, before, after)


def local_apply_kernel(
    tab_ref, tensor_ref, back_hbm, own_ref, field_ref, a_ref, at_ref, col_a, col_b, slots, sems, *, start
):
    width = own_ref.shape[1]
    tiles = field_ref.shape[0] // 24 - 1
    inner = tab_ref[0, 0]
    stream = Stream(back_hbm, slots, sems, MATS * width, SLOTS, True)
    stream.start(0, jnp.minimum(rounded(inner), SLOTS))
    field_ref[...] = jnp.zeros_like(field_ref)
    a_ref[...] = jnp.zeros_like(a_ref)
    split_rows(a_ref, 0, own_ref, start, tiles, 3)
    turn_rows(at_ref, a_ref)
    select = selector(3, width)
    cols = (col_a, col_b)
    apply_jobs(tab_ref, 1, tiles + inner, at_ref, 0, cols, select, field_ref, tensor_ref)
    apply_jobs(tab_ref, 3, inner, at_ref, 0, cols, select, field_ref, slots, stream)


def cross_apply_kernel(
    par_ref, own_tab, prev_tab, tensor_ref, prev_hbm, own_ref, near_ref, far_ref, inv_ref, part_ref,
    out_ref, field_ref, a_ref, at_ref, col_a, col_b, slots, sems,
    *, start, inv_start,
):
    width = own_ref.shape[1]
    tiles = out_ref.shape[0] // 3
    behind = prev_tab[0, 0]
    stream = Stream(prev_hbm, slots, sems, MATS * width, SLOTS, True)
    stream.start(0, jnp.minimum(rounded(behind), SLOTS))
    par = par_ref[0]
    field_ref[...] = part_ref[...]
    a_ref[...] = jnp.zeros_like(a_ref)
    split_rows(a_ref, par * tiles, near_ref, start, tiles, 3)
    split_rows(a_ref, (1 - par) * tiles, far_ref, start, tiles, 3)
    turn_rows(at_ref, a_ref)
    select = selector(3, width)
    cols = (col_a, col_b)
    apply_jobs(own_tab, 2, own_tab[0, 1], at_ref, 0, cols, select, field_ref, tensor_ref)
    apply_jobs(prev_tab, 1, behind, at_ref, tiles, cols, select, field_ref, slots, stream)
    for t in range(tiles):
        weight = (inv_ref[inv_start + t : inv_start + t + 1, :] - SHIFT) * (1.0 / SCALE)
        for c in range(3):
            at = c * tiles + t
            field = jnp.sum(field_ref[(t * 3 + c) * 8 : (t * 3 + c) * 8 + 8, :], axis=0, keepdims=True)
            mine = own_ref[start + at : start + at + 1, :]
            out_ref[at : at + 1, :] = mine * weight - field * (1.0 / SCALE)


PAIRS = [(i, j) for i in range(ITERS + 1) for j in range(i, ITERS + 1)]


def gram_kernel(*refs, start):
    vectors, out_ref = refs[:-1], refs[-1]
    rows, width = vectors[-1].shape
    lane = lax.broadcasted_iota(jnp.int32, (1, width), 1)
    total = jnp.zeros((1, width), F32)
    starts = (start,) + (0,) * ITERS
    for n, (i, j) in enumerate(PAIRS):
        product = vectors[i][starts[i] : starts[i] + rows, :] * vectors[j][starts[j] : starts[j] + rows, :]
        line = jnp.sum(product, axis=0, keepdims=True)
        total = jnp.where(lane == n, jnp.sum(line, axis=1, keepdims=True), total)
    out_ref[...] = total


def untile_kernel(inv_ref, *refs, start):
    vectors, outs = refs[: ITERS + 1], refs[ITERS + 1 :]
    tiles, width = inv_ref.shape
    starts = (start,) + (0,) * ITERS
    zero = jnp.zeros((8, width), F32)
    for q in range(tiles // 8):
        index = inv_ref[8 * q : 8 * q + 8, :]
        high = index // width
        low = index - high * width

        def step(h, acc):
            hit = high == h
            return tuple(
                jnp.where(hit, lane_pick(spread(vectors[n // 3][pl.ds(starts[n // 3] + n % 3 * tiles + h, 1), :]), low), acc[n])
                for n in range(3 * (ITERS + 1))
            )

        acc = lax.fori_loop(0, tiles, step, (zero,) * (3 * (ITERS + 1)), unroll=8)
        for n in range(3 * (ITERS + 1)):
            for s in range(8):
                at = (8 * q + s) * width
                outs[n // 3][n % 3 : n % 3 + 1, at : at + width] = acc[n][s : s + 1, :]


def output_kernel(parts_ref, *refs):
    vectors, (dip_ref, res_ref) = refs[: ITERS + 1], refs[ITERS + 1 :]
    width = parts_ref.shape[1]
    sums = jnp.sum(parts_ref[...], axis=0, keepdims=True)
    lane = lax.broadcasted_iota(jnp.int32, (1, width), 1)
    gram = {}
    for n, (i, j) in enumerate(PAIRS):
        value = jnp.sum(jnp.where(lane == n, sums, 0.0), axis=1, keepdims=True)
        gram[i, j] = gram[j, i] = jnp.broadcast_to(value, (1, width))

    def add(a, b):
        return b if a is None else a if b is None else a + b

    def inner(a, b):
        total = None
        for i in range(ITERS + 1):
            line = None
            for j in range(ITERS + 1):
                if a[i] is not None and b[j] is not None:
                    line = add(line, b[j] * gram[i, j])
            if line is not None:
                total = add(total, a[i] * line)
        return total

    def operate(a):
        out = [None if v is None else SHIFT * v for v in a]
        for i in range(ITERS):
            if a[i] is not None:
                out[i + 1] = add(out[i + 1], SCALE * a[i])
        return out

    x = [None] * (ITERS + 1)
    r = [jnp.ones((1, width), F32)] + [None] * ITERS
    d = list(r)
    norm = inner(r, r)
    for step in range(ITERS):
        q = operate(d)
        size = norm / inner(d, q)
        x = [add(x[k], None if d[k] is None else size * d[k]) for k in range(ITERS + 1)]
        r = [add(r[k], None if q[k] is None else -size * q[k]) for k in range(ITERS + 1)]
        if step + 1 < ITERS:
            new = inner(r, r)
            ratio = new / norm
            d = [add(r[k], None if d[k] is None else ratio * d[k]) for k in range(ITERS + 1)]
            norm = new
    x = [None if v is None else jnp.broadcast_to(v, (3, width)) for v in x]
    r = [jnp.broadcast_to(v, (3, width)) for v in r]
    for b in range(dip_ref.shape[1] // width):
        at = slice(b * width, (b + 1) * width)
        values = [vectors[k][:, at] for k in range(ITERS + 1)]
        for out, weights in ((dip_ref, x), (res_ref, r)):
            total = None
            for k in range(ITERS + 1):
                if weights[k] is not None:
                    total = add(total, weights[k] * values[k])
            out[:, at] = total


def shape(rows, width, dtype=F32):
    return jax.ShapeDtypeStruct((rows, width), dtype)


def cost(flops):
    return pl.CostEstimate(flops=flops, bytes_accessed=1_000_000, transcendentals=0)


def on_device(positions, polar, field_ext, tile_atom, tile_list, image_shift):
    tiles, links = tile_list.shape
    atoms = tile_atom.shape[0]
    width = atoms // tiles
    slabs = lax.axis_size("gx")
    slab = lax.axis_index("gx")
    rows = 3 * tiles
    cap = tiles * (links - 1)
    size = MATS * width
    boxes = (4.0 * slabs, 128.0, 2.0 * tiles)
    near_pairs = [(i, i ^ 1) for i in range(slabs)]
    far_pairs = [(i, ((i + 1) ^ 1) - 1 if 0 < i < slabs - 1 else slabs - 1 - i) for i in range(slabs)]
    ahead = [(i, (i + 1) % slabs) for i in range(slabs)]

    def swap(value):
        return lax.ppermute(value, "gx", far_pairs), lax.ppermute(value, "gx", near_pairs)

    own_list = tile_list.T
    own_shift = image_shift.transpose(2, 0, 1)
    prev_list = lax.ppermute(own_list, "gx", ahead)
    prev_shift = lax.ppermute(own_shift, "gx", ahead)
    par = jnp.stack([slab % 2, (slab == slabs - 1).astype(jnp.int32), (slab == 0).astype(jnp.int32)])
    par = par.astype(jnp.int32)
    index = tile_atom.reshape(tiles, width)
    packed = pl.pallas_call(
        tile_in_kernel,
        out_shape=shape(8 * tiles, width),
        in_specs=[HBM] * 4,
        out_specs=VMEM,
        scratch_shapes=[
            pltpu.VMEM((3, atoms), F32),
            pltpu.VMEM((1, atoms), F32),
            pltpu.VMEM((3, atoms), F32),
            pltpu.VMEM((tiles, width), jnp.int32),
            pltpu.SemaphoreType.DMA((4,)),
        ],
        compiler_params=params(4),
        name="tile_in",
    )(*(pltpu.with_memory_space_constraint(v, pltpu.MemorySpace.HBM) for v in (positions, polar.reshape(1, -1), field_ext, index)))
    far, near = swap(packed)
    inverse = pl.pallas_call(
        inverse_kernel,
        out_shape=shape(tiles, width, jnp.int32),
        in_specs=[VMEM],
        out_specs=VMEM,
        compiler_params=params(4),
        cost_estimate=cost(4_000_000),
        name="inverse",
    )(index)
    table = shape(4, tiles + cap + PAD, jnp.int32)
    tensor_shape = pltpu.VMEM(((tiles + cap + 1) * size, width), F32)
    stream_shape = pltpu.MemorySpace.HBM(((cap + BATCH) * size, width), F32)

    def scratch(groups, comps, depth):
        col = pltpu.VMEM((HALF * width, comps * width), F32)
        return [
            pltpu.VMEM((groups * tiles * GROUP, width), F32),
            pltpu.VMEM((groups * tiles * width, GROUP), jnp.bfloat16),
            col,
            col,
            pltpu.VMEM((depth * size, width), F32),
            pltpu.SemaphoreType.DMA((depth,)),
        ]

    tensor, back_tensor, own_tab = pl.pallas_call(
        functools.partial(local_pairs_kernel, boxes=boxes),
        out_shape=(tensor_shape, stream_shape, table),
        in_specs=[SMEM, SMEM, VMEM],
        out_specs=(VMEM, HBM, SMEM),
        scratch_shapes=scratch(1, 4, OUT_SLOTS),
        compiler_params=params(12),
        cost_estimate=cost(60_000_000),
        name="local_pairs",
    )(own_list, own_shift, packed)
    tensor, prev_tensor, prev_tab = pl.pallas_call(
        functools.partial(cross_pairs_kernel, boxes=boxes),
        out_shape=(tensor_shape, stream_shape, table),
        in_specs=[SMEM] * 4 + [VMEM] * 4,
        out_specs=(VMEM, HBM, SMEM),
        scratch_shapes=scratch(2, 4, OUT_SLOTS),
        input_output_aliases={7: 0},
        compiler_params=params(12),
        cost_estimate=cost(60_000_000),
        name="cross_pairs",
    )(par, own_tab, prev_list, prev_shift, packed, near, far, tensor)
    prev_tensor = pltpu.with_memory_space_constraint(prev_tensor, pltpu.MemorySpace.HBM)
    back_tensor = pltpu.with_memory_space_constraint(back_tensor, pltpu.MemorySpace.HBM)
    fields = 24 * (tiles + 1)

    def apply(vector, near, far, start):
        part = pl.pallas_call(
            functools.partial(local_apply_kernel, start=start),
            out_shape=shape(fields, width),
            in_specs=[SMEM, VMEM, HBM, VMEM],
            out_specs=VMEM,
            scratch_shapes=scratch(1, 3, SLOTS),
            compiler_params=params(12),
            cost_estimate=cost(60_000_000),
            name="local_apply",
        )(own_tab, tensor, back_tensor, vector)
        return pl.pallas_call(
            functools.partial(cross_apply_kernel, start=start, inv_start=7 * tiles),
            out_shape=shape(rows, width),
            in_specs=[SMEM] * 3 + [VMEM, HBM] + [VMEM] * 5,
            out_specs=VMEM,
            scratch_shapes=[pltpu.VMEM((fields, width), F32)] + scratch(2, 3, SLOTS),
            compiler_params=params(12),
            cost_estimate=cost(60_000_000),
            name="cross_apply",
        )(par, own_tab, prev_tab, tensor, prev_tensor, vector, near, far, packed, part)

    start = 4 * tiles
    basis = [packed]
    vector = apply(packed, near, far, start)
    basis.append(vector)
    for _ in range(ITERS - 1):
        far, near = swap(vector)
        vector = apply(vector, near, far, 0)
        basis.append(vector)
    gram = pl.pallas_call(
        functools.partial(gram_kernel, start=start),
        out_shape=shape(1, width),
        in_specs=[VMEM] * (ITERS + 1),
        out_specs=VMEM,
        compiler_params=params(4),
        name="gram",
    )(*basis)
    parts = lax.all_to_all(jnp.broadcast_to(gram, (slabs, width)), "gx", 0, 0, tiled=True)
    natural = pl.pallas_call(
        functools.partial(untile_kernel, start=start),
        out_shape=(shape(3, atoms),) * (ITERS + 1),
        in_specs=[VMEM] * (ITERS + 2),
        out_specs=(VMEM,) * (ITERS + 1),
        compiler_params=params(4),
        cost_estimate=cost(60_000_000),
        name="untile",
    )(inverse, *basis)
    return pl.pallas_call(
        output_kernel,
        out_shape=(shape(3, atoms), shape(3, atoms)),
        in_specs=[VMEM] * (ITERS + 2),
        out_specs=(VMEM, VMEM),
        compiler_params=params(4),
        name="outputs",
    )(parts, *natural)


def solution(mesh):
    return jax.shard_map(
        on_device,
        mesh=mesh,
        in_specs=(
            P(None, REP_GX),
            P(REP_GX),
            P(None, REP_GX),
            P(REP_GX),
            P(REP_GX, None),
            P(None, REP_GX, None),
        ),
        out_specs=(P(None, REP_GX), P(None, REP_GX)),
        check_vma=False,
    )
```
